8 devices in a mesh: dp: 2 (over y, z), tp: 4 (over x, core).
Axes of the slice: x: 2, y: 2, z: 1, core: 2. Of those that a mesh axis runs over, the one named last changes fastest.
Arguments:
- x: bfloat16 [2816, 3072], P(('dp', 'tp')), parts along dimension 0
- dy: bfloat16 [2816, 3072], P(('dp', 'tp')), parts along dimension 0
- gate: bfloat16 [2816, 8192], P('dp', 'tp'), parts along dimension 0
- up: bfloat16 [2816, 8192], P('dp', 'tp'), parts along dimension 0
- w_gate: bfloat16 [3072, 8192], P(None, 'tp')
- w_up: bfloat16 [3072, 8192], P(None, 'tp')
- w_down: bfloat16 [8192, 3072], P('tp')
Outputs:
- output 1: bfloat16 [2816, 3072], P(('dp', 'tp')), parts along dimension 0
- output 2: bfloat16 [6144, 8192], P('dp', 'tp'), parts along dimension 0
- output 3: bfloat16 [6144, 8192], P('dp', 'tp'), parts along dimension 0
- output 4: bfloat16 [16384, 3072], P(('dp', 'tp')), parts along dimension 0
There are 2 independent parts. The reference program is written for one: setup_inputs(seed, part) draws one part's arguments, and reference() takes and returns one part's arrays. A program takes and returns all parts, laid end to end along the dimension named above; an argument that names none is the same for every part.
All inputs are finite; a program needn't handle non-finite values.
Results may differ from the reference program's by a relative error of at most 0.012.
Values are sent between devices in bfloat16 or wider.
A program may use at most 2 GiB of HBM per device.

```python
import jax
import jax.numpy as jnp

ROWS = 1408
D = 3072
FF = 8192


def act(gate, up):
    return jax.nn.silu(gate) * up


def setup_inputs(seed: int = 0, part: int = 0) -> dict:
    kx, ky, ka, kb, kg, ku, kd = jax.random.split(jax.random.key(seed), 7)
    kx, ky, ka, kb = (jax.random.fold_in(k, part) for k in (kx, ky, ka, kb))
    drawn = {
        "x": jax.random.normal(kx, (ROWS, D), jnp.float32),
        "dy": jax.random.normal(ky, (ROWS, D), jnp.float32),
        "gate": jax.random.normal(ka, (ROWS, FF), jnp.float32),
        "up": jax.random.normal(kb, (ROWS, FF), jnp.float32),
        "w_gate": jax.random.normal(kg, (D, FF), jnp.float32) * D**-0.5,
        "w_up": jax.random.normal(ku, (D, FF), jnp.float32) * D**-0.5,
        "w_down": jax.random.normal(kd, (FF, D), jnp.float32) * FF**-0.5,
    }
    return {k: v.astype(jnp.bfloat16) for k, v in drawn.items()}


def reference(x, dy, gate, up, w_gate, w_up, w_down):
    hidden, back = jax.vjp(act, gate.astype(jnp.float32), up.astype(jnp.float32))
    d_hidden = jnp.dot(dy, w_down.T, preferred_element_type=jnp.float32)
    d_gate, d_up = (g.astype(jnp.bfloat16) for g in back(d_hidden))
    dx = jnp.dot(d_gate, w_gate.T, preferred_element_type=jnp.float32) + jnp.dot(d_up, w_up.T, preferred_element_type=jnp.float32)
    dw_gate = jnp.dot(x.T, d_gate, preferred_element_type=jnp.float32)
    dw_up = jnp.dot(x.T, d_up, preferred_element_type=jnp.float32)
    dw_down = jnp.dot(hidden.astype(jnp.bfloat16).T, dy, preferred_element_type=jnp.float32)
    return tuple(g.astype(jnp.bfloat16) for g in (dx, dw_gate, dw_up, dw_down))
```

```python
import functools

import jax
import jax.numpy as jnp
from jax import lax
from jax.experimental import pallas as pl
from jax.experimental.pallas import tpu as pltpu
from jax.sharding import PartitionSpec as P

F32 = jnp.float32
BF16 = jnp.bfloat16
DMA = pltpu.SemaphoreType.DMA
ANY = pl.BlockSpec(memory_space=pl.ANY)
VMEM_LIMIT = 60 * 2**20


def nt(a, b):
    return lax.dot_general(a, b, (((1,), (1,)), ((), ())), preferred_element_type=F32)


def tn(a, b):
    return lax.dot_general(a, b, (((0,), (0,)), ((), ())), preferred_element_type=F32)


def hidden_grads_kernel(dy_a, dy_b, w_down, gate, up, w_gate, w_up, *rest, slot, row, bn, bx, n_alias):
    (d_gate, d_up, hidden, keep, send), scratch = rest[n_alias : n_alias + 5], rest[n_alias + 5 :]
    (dyv, wdb, gb, ub, da, db, dgv, duv, hv, wgb, wub, kb, sb, s_dy, s_w, s_g, s_u, s_x, s_o, s_k, s_s) = scratch
    rows, depth = dyv.shape
    half = rows // 2
    ff = w_down.shape[0]
    steps, blocks = ff // bn, depth // bx
    sub = bn // 2
    me = lax.axis_index("tp")

    def at(k):
        return pl.multiple_of(row(me, k), 16)

    def dy_copy(k):
        return pltpu.make_async_copy((dy_a, dy_b)[k], dyv.at[pl.ds(k * half, half)], s_dy.at[k])

    def w_copy(j, b):
        return pltpu.make_async_copy(w_down.at[pl.ds(pl.multiple_of(j * bn, bn), bn)], wdb.at[b], s_w.at[b])

    def act_copies(j, b):
        cols = pl.ds(pl.multiple_of(j * bn, bn), bn)
        return [
            pltpu.make_async_copy(src.at[pl.ds(at(k), half), cols], buf.at[b, pl.ds(k * half, half)], sem.at[b, k])
            for src, buf, sem in ((gate, gb, s_g), (up, ub, s_u))
            for k in range(2)
        ]

    def x_copies(i, b):
        r = pl.ds(pl.multiple_of(i * bx, bx), bx)
        return [
            pltpu.make_async_copy(w_gate.at[r], wgb.at[b], s_x.at[0, b]),
            pltpu.make_async_copy(w_up.at[r], wub.at[b], s_x.at[1, b]),
        ]

    def out_copies(i, b):
        c = pl.ds(pl.multiple_of(i * bx, bx), bx)
        return [
            pltpu.make_async_copy(kb.at[b], keep.at[:, c], s_k.at[b]),
            pltpu.make_async_copy(sb.at[b], send.at[:, c], s_s.at[b]),
        ]

    def epilogue(d, j, b, part):
        s = pl.ds(part * sub, sub)
        g, u = gb[b, :, s].astype(F32), ub[b, :, s].astype(F32)
        sig = 1.0 / (1.0 + jnp.exp(-g))
        silu = g * sig
        dh = d[...]
        o = pl.ds(pl.multiple_of(j * bn + part * sub, sub), sub)
        hv[:, o] = (silu * u).astype(BF16)
        duv[:, o] = (dh * silu).astype(BF16)
        dgv[:, o] = ((dh * u) * (sig + silu * (1.0 - sig))).astype(BF16)

    def start(copies):
        for c in copies:
            c.start()

    def wait(copies):
        for c in copies:
            c.wait()

    dy_copy(0).start()
    dy_copy(1).start()
    w_copy(0, 0).start()
    start(act_copies(0, 0))
    dy_copy(0).wait()
    dy_copy(1).wait()

    def step(j, carry):
        b, b3 = lax.rem(j, 2), lax.rem(j, 3)
        w_copy(j, b).wait()
        wait(act_copies(j, b3))

        @pl.when(j + 1 < steps)
        def _():
            w_copy(j + 1, 1 - b).start()
            start(act_copies(j + 1, lax.rem(j + 1, 3)))

        @pl.when(j + 1 == steps)
        def _():
            start(x_copies(0, 0))

        da[...] = nt(dyv[...], wdb[b, pl.ds(0, sub)])
        epilogue(db, jnp.maximum(j - 1, 0), lax.rem(j + 2, 3), 1)
        db[...] = nt(dyv[...], wdb[b, pl.ds(sub, sub)])
        epilogue(da, j, b3, 0)
        return carry

    lax.fori_loop(0, steps, step, 0)
    epilogue(db, steps - 1, (steps - 1) % 3, 1)
    saved = [
        pltpu.make_async_copy(v, o.at[pl.ds(slot, rows)], s_o.at[n])
        for n, (v, o) in enumerate(((dgv, d_gate), (duv, d_up), (hv, hidden)))
    ]
    start(saved)

    def block(i, carry):
        b = lax.rem(i, 2)
        wait(x_copies(i, b))

        @pl.when(i + 1 < blocks)
        def _():
            start(x_copies(i + 1, 1 - b))

        @pl.when(i >= 2)
        def _():
            wait(out_copies(i - 2, b))

        t = nt(dgv[...], wgb[b]) + nt(duv[...], wub[b])
        kb[b] = t[:half]
        sb[b] = t[half:].astype(BF16)
        start(out_copies(i, b))
        return carry

    lax.fori_loop(0, blocks, block, 0)
    for i in (blocks - 2, blocks - 1):
        wait(out_copies(i, i % 2))
    wait(saved)


def hidden_grads(dy_a, dy_b, w_down, gate, up, w_gate, w_up, into, *, slot, row, bn=512, bx=512, name):
    half, depth = dy_a.shape
    rows, (total, ff) = 2 * half, gate.shape
    S = jax.ShapeDtypeStruct
    n_alias = len(into)
    V = pltpu.VMEM
    return pl.pallas_call(
        functools.partial(hidden_grads_kernel, slot=slot, row=row, bn=bn, bx=bx, n_alias=n_alias),
        in_specs=[ANY] * (7 + n_alias),
        out_specs=[ANY] * 5,
        out_shape=[S((total, ff), BF16)] * 3 + [S((half, depth), F32), S((half, depth), BF16)],
        scratch_shapes=[
            V((rows, depth), BF16), V((2, bn, depth), BF16), V((3, rows, bn), BF16), V((3, rows, bn), BF16),
            V((rows, bn // 2), F32), V((rows, bn // 2), F32), V((rows, ff), BF16), V((rows, ff), BF16), V((rows, ff), BF16),
            V((2, bx, ff), BF16), V((2, bx, ff), BF16), V((2, half, bx), F32), V((2, half, bx), BF16),
            DMA((2,)), DMA((2,)), DMA((3, 2)), DMA((3, 2)), DMA((2, 2)), DMA((3,)), DMA((2,)), DMA((2,)),
        ],
        input_output_aliases={7 + n: n for n in range(n_alias)},
        compiler_params=pltpu.CompilerParams(vmem_limit_bytes=VMEM_LIMIT),
        cost_estimate=pl.CostEstimate(
            flops=6 * rows * depth * ff, bytes_accessed=6 * depth * ff, transcendentals=rows * ff
        ),
        name=name,
    )(dy_a, dy_b, w_down, gate, up, w_gate, w_up, *into)


def weight_grads_kernel(*refs, left, right, n_left, n_right, n_out, bm, bc):
    lefts, rights = refs[:n_left], refs[n_left : n_left + n_right]
    outs = refs[n_left + n_right : n_left + n_right + n_out]
    lb, rv, ob, s_l, s_r, s_o = refs[n_left + n_right + n_out :]
    m = lefts[0].shape[1]
    n = rv.shape[2]
    blocks, chunks = m // bm, n // bc

    def l_copies(i, b):
        c = pl.ds(pl.multiple_of(i * bm, bm), bm)
        return [
            pltpu.make_async_copy(
                lefts[p].at[pl.ds(r0, rows), c], lb.at[b, pl.ds(to, rows)], s_l.at[b, k]
            )
            for k, (p, r0, to, rows) in enumerate(left)
        ]

    def r_copies(r, c):
        cc = pl.ds(c * bc, bc)
        return [
            pltpu.make_async_copy(
                rights[p].at[pl.ds(r0, rows), cc], rv.at[r, pl.ds(to, rows), cc], s_r.at[r, c, k]
            )
            for k, (p, r0, to, rows) in enumerate(right[r])
        ]

    def o_copy(r, i, b):
        return pltpu.make_async_copy(ob.at[b, r], outs[r].at[pl.ds(pl.multiple_of(i * bm, bm), bm)], s_o.at[b, r])

    def start(copies):
        for c in copies:
            c.start()

    def wait(copies):
        for c in copies:
            c.wait()

    pieces = [(r, c) for r in range(n_out) for c in range(chunks)]
    start(l_copies(0, 0))
    for r, c in pieces:
        start(r_copies(r, c))

    wait(l_copies(0, 0))
    start(l_copies(1, 1))
    for r, c in pieces:
        wait(r_copies(r, c))
        cc = pl.ds(c * bc, bc)
        ob[0, r, :, cc] = tn(lb[0], rv[r, :, cc]).astype(BF16)
    for r in range(n_out):
        o_copy(r, 0, 0).start()

    def block(i, carry):
        b = lax.rem(i, 2)
        wait(l_copies(i, b))

        @pl.when(i + 1 < blocks)
        def _():
            start(l_copies(i + 1, 1 - b))

        @pl.when(i >= 2)
        def _():
            for r in range(n_out):
                o_copy(r, i - 2, b).wait()

        for r in range(n_out):
            ob[b, r] = tn(lb[b], rv[r]).astype(BF16)
        for r in range(n_out):
            o_copy(r, i, b).start()
        return carry

    lax.fori_loop(1, blocks, block, 0)
    for i in (blocks - 2, blocks - 1):
        for r in range(n_out):
            o_copy(r, i, i % 2).wait()


def weight_grads(lefts, left, rights, right, *, bm, bc, name):
    n_out = len(right)
    total = sum(p[3] for p in left)
    m, n = lefts[0].shape[1], rights[0].shape[1]
    V = pltpu.VMEM
    return pl.pallas_call(
        functools.partial(
            weight_grads_kernel, left=left, right=right, n_left=len(lefts), n_right=len(rights), n_out=n_out, bm=bm, bc=bc
        ),
        in_specs=[ANY] * (len(lefts) + len(rights)),
        out_specs=[ANY] * n_out,
        out_shape=[jax.ShapeDtypeStruct((m, n), BF16)] * n_out,
        scratch_shapes=[
            V((2, total, bm), BF16), V((n_out, total, n), BF16), V((2, n_out, bm, n), BF16),
            DMA((2, len(left))), DMA((n_out, n // bc, max(len(r) for r in right))), DMA((2, n_out)),
        ],
        compiler_params=pltpu.CompilerParams(vmem_limit_bytes=VMEM_LIMIT),
        cost_estimate=pl.CostEstimate(flops=2 * n_out * total * m * n, bytes_accessed=2 * n_out * m * n, transcendentals=0),
        name=name,
    )(*lefts, *rights)


def finish_kernel(chip, part, *rest):
    out = rest[-1]
    out[...] = (chip[...] + part[...].astype(F32)).astype(BF16)


def finish(chip, part, k, into, *, name):
    h, depth = part.shape
    bc = 1024
    whole = pl.BlockSpec((h, bc), lambda c: (k, c))
    return pl.pallas_call(
        finish_kernel,
        grid=(depth // bc,),
        in_specs=[whole, pl.BlockSpec((h, bc), lambda c: (0, c))] + [ANY] * len(into),
        out_specs=whole,
        out_shape=jax.ShapeDtypeStruct(chip.shape, BF16),
        input_output_aliases={2: 0} if into else {},
        cost_estimate=pl.CostEstimate(flops=h * depth, bytes_accessed=8 * h * depth, transcendentals=0),
        compiler_params=pltpu.CompilerParams(vmem_limit_bytes=16 * 2**20),
        name=name,
    )(chip, part, *into)


def solution(mesh):
    mate = [(i, i ^ 1) for i in range(4)]
    across = [(i, i ^ 2) for i in range(4)]

    def step(x, dy, gate, up, w_gate, w_up, w_down):
        own = dy.shape[0]
        h = own // 2
        to_mate = lambda a: lax.ppermute(a, "tp", mate)
        to_across = lambda a: lax.ppermute(a, "tp", across)
        tie = lax.optimization_barrier

        dy_q = [to_across(dy[k * h : (k + 1) * h]) for k in range(2)]
        dy_mate = to_mate(dy)
        x_q = [to_across(x[k * h : (k + 1) * h]) for k in range(2)]
        x_mate = to_mate(x)

        weights = (w_down, gate, up, w_gate, w_up)
        *saved, keep, send = hidden_grads(
            dy, dy_mate, *weights, (), slot=0, row=lambda me, k: (me ^ k) * own, name="local"
        )
        parts, dy_r, x_r = [], [None] * 2, [None] * 2
        q, saved, keep, send = tie((dy_q[0], saved, keep, send))
        dy_q[0], dy_r[0] = q, to_mate(q)
        chip = keep + to_mate(send).astype(F32)
        for k in range(2):
            saved, chip, dy_r[k] = tie((saved, chip, dy_r[k]))
            *saved, keep, send = hidden_grads(
                dy_q[k], dy_r[k], *weights, saved, slot=2 * own + 2 * h * k,
                row=lambda me, s, k=k: (me ^ 2 ^ s) * own + k * h, name=f"remote{k}",
            )
            if k == 0:
                q, saved, keep, send = tie((dy_q[1], saved, keep, send))
                dy_q[1], dy_r[1] = q, to_mate(q)
            else:
                q, saved, keep, send = tie((x_q[0], saved, keep, send))
                x_q[0], x_r[0] = q, to_mate(q)
            pair = (keep + to_mate(send).astype(F32)).astype(BF16)
            parts.append(to_across(pair))
        d_gate, d_up, hidden = saved

        slots = [(0, 0, 0, own), (1, 0, own, own)]
        dy_slots = slots + [(2 + i, 0, 2 * own + i * h, h) for i in range(4)]
        whole = [(0, 0, 0, 4 * own)]
        hidden, x_r[0] = tie((hidden, x_r[0]))
        (dw_down,) = weight_grads(
            (hidden,), whole, (dy, dy_mate, dy_q[0], dy_r[0], dy_q[1], dy_r[1]), [dy_slots], bm=512, bc=1024, name="down"
        )
        q, dw_down, d_gate, d_up = tie((x_q[1], dw_down, d_gate, d_up))
        x_q[1], x_r[1] = q, to_mate(q)
        dw_gate, dw_up = weight_grads(
            (x, x_mate, x_q[0], x_r[0], x_q[1], x_r[1]), dy_slots, (d_gate, d_up), [whole, [(1, 0, 0, 4 * own)]], bm=512,
            bc=1024, name="gateup"
        )
        parts, chip, dw_gate, dw_up = tie((parts, chip, dw_gate, dw_up))
        dx = finish(chip, parts[0], 0, (), name="finish0")
        dx = finish(chip, parts[1], 1, (dx,), name="finish1")
        return dx, dw_gate, dw_up, dw_down

    rows, cols = P(("dp", "tp"), None), P("dp", "tp")
    return jax.shard_map(
        step,
        mesh=mesh,
        in_specs=(rows, rows, cols, cols, P(None, "tp"), P(None, "tp"), P("tp", None)),
        out_specs=(rows, cols, cols, rows),
        check_vma=False,
    )
```
